256 devices in a mesh: vp: 64 (over y, z, core), rep: 4 (over x).
Axes of the slice: x: 4, y: 4, z: 8, core: 2. Of those that a mesh axis runs over, the one named last changes fastest.
Arguments:
- features: bfloat16 [524288, 256], P(('vp', 'rep')), may hold values from -48 to 48
- tile_values: bfloat16 [65536, 128, 128], P(('vp', 'rep')), may hold values from 0 to 0.0014648438
- tile_cols: int32 [65536], P(('vp', 'rep')), may hold values from 0 to 31, as said below
- halo_rows: int32 [256, 4, 4], P(('vp', 'rep')), may hold values from 0 to 15
Outputs:
- scores: bfloat16 [524288, 256], P(('vp', 'rep'))
The draws below stay inside these ranges and needn't reach their ends.
Inputs may be any that keep to these rules, and one draw needn't show every extreme that they name: `tile_cols`: values below 16 name one of the shard's own row blocks; value 16 + o * 4 + j names the j-th block sent by peer o. Every value occurs on every shard.
All inputs are finite; a program needn't handle non-finite values.
Results may differ from the reference program's by a relative error of at most 0.002.
Values may be sent and summed in bfloat16 or wider, within the bound.
No kernel may reach another device: no remote copies, remote signals or barrier semaphores. Data moves between devices by JAX's collectives and lax.ppermute only.
A program may use at most 128 MiB of HBM per device.

```python
import math
import jax
import jax.numpy as jnp
from jax import lax

CLASSES = 256
TILE = 128
BLOCKS_DEV = 16
TILES_ROW = 16
HALO_SLOTS = 4
ITERS = 3
SHARDS = 256
VERTICES = 524288
TILES = 65536


def draw_features(key, part):
    scale_key, noise_key, common_key = jax.random.split(key, 3)
    block_count = SHARDS * BLOCKS_DEV
    scales = jnp.exp(jax.random.uniform(scale_key, (block_count, 1, 1), minval=0.0, maxval=math.log(8.0)))
    noise = jnp.clip(jax.random.normal(noise_key, (block_count, TILE, CLASSES)), -6.0, 6.0)
    values = scales * noise
    values = jnp.clip(values, -48.0, 48.0).reshape(block_count * TILE, CLASSES)
    return values.astype(jnp.bfloat16)


def draw_tile_cols(key, part):
    slot_count = BLOCKS_DEV + 4 * HALO_SLOTS
    per_device = BLOCKS_DEV * TILES_ROW
    device_keys = jax.random.split(key, SHARDS)

    def one_device(device_key):
        first_key, second_key = jax.random.split(device_key)
        base_slots = jax.random.randint(first_key, (per_device,), 0, slot_count, dtype=jnp.int32)
        placing = jax.random.permutation(second_key, per_device)
        return base_slots.at[placing[:slot_count]].set(jnp.arange(slot_count, dtype=jnp.int32))
    return jax.vmap(one_device)(device_keys).reshape(-1)


def with_ends(entries, key, least, top_value):
    index_at = [jax.random.randint(jax.random.fold_in(key, axis), (), 0, length) for axis, length in enumerate(entries.shape)]
    main_axis = entries.shape.index(max(entries.shape))
    next_to = index_at[:main_axis] + [(index_at[main_axis] + 1) % entries.shape[main_axis]] + index_at[main_axis + 1:]
    return entries.at[tuple(index_at)].set(least).at[tuple(next_to)].set(top_value)


def levels(key, extent, cuts, least, largest):
    gain, own = 1.0, jax.random.fold_in(key, 6)
    for dim, parts in cuts:
        heights = jnp.exp(jax.random.uniform(jax.random.fold_in(own, dim), (parts,), jnp.float32, least / len(cuts), largest / len(cuts)))
        gain = gain * jnp.repeat(heights, extent[dim] // parts).reshape([-1 if axis == dim else 1 for axis in range(len(extent))])
    return gain


def setup_inputs(seed: int = 0) -> dict:
    seeds = jax.random.split(jax.random.key(seed), 5)
    return {
        "features": draw_features(jax.random.fold_in(seeds[4], 71), 0),
        "tile_values": jnp.clip(0.0014648438 * jax.random.uniform(seeds[1], (TILES, TILE, TILE), jnp.float32) ** levels(seeds[1], (TILES, TILE, TILE), ((0, 256),), -0.2, 0.2), 0.0, 0.0014648438).astype(jnp.bfloat16),
        "tile_cols": draw_tile_cols(jax.random.fold_in(seeds[4], 71), 0),
        "halo_rows": with_ends(jax.random.randint(seeds[3], (SHARDS, 4, HALO_SLOTS), 0, BLOCKS_DEV), jax.random.fold_in(seeds[3], 1), 0, BLOCKS_DEV - 1).astype(jnp.int32),
    }


def reference(features, tile_values, tile_cols, halo_rows):
    nblocks = BLOCKS_DEV
    tiles_dev = BLOCKS_DEV * TILES_ROW
    device_ids = jnp.arange(SHARDS, dtype=jnp.int32)
    slots = tile_cols.reshape(SHARDS, tiles_dev).astype(jnp.int32)
    is_local = slots < nblocks
    halo_slot = jnp.maximum(slots - nblocks, 0)
    offset_slot = (halo_slot // HALO_SLOTS).astype(jnp.int32)
    slot_entry = (halo_slot % HALO_SLOTS).astype(jnp.int32)
    shift_by = jnp.array([1, -1, 4, -4], dtype=jnp.int32)[offset_slot]
    sender = ((device_ids[:, None] - shift_by) % SHARDS).astype(jnp.int32)
    sent_block = halo_rows[sender, offset_slot, slot_entry].astype(jnp.int32)
    source_block = jnp.where(is_local, device_ids[:, None] * nblocks + slots, sender * nblocks + sent_block).astype(jnp.int32)
    source_block = source_block.reshape(SHARDS, nblocks, TILES_ROW)
    tiles = tile_values.reshape(SHARDS, nblocks, TILES_ROW, TILE, TILE)
    teleport_part = 0.1 * features.astype(jnp.float32)
    current = features
    for iteration in range(ITERS):
        blocks = current.reshape(SHARDS * nblocks, TILE, CLASSES)

        def propagate_device(pair):
            tiles_here, sources_here = pair
            gathered = blocks[sources_here]
            return jnp.einsum('rtij,rtjc->ric', tiles_here.astype(jnp.float32), gathered.astype(jnp.float32), precision=lax.Precision.HIGHEST)
        propagated = lax.map(propagate_device, (tiles, source_block)).reshape(VERTICES, CLASSES)
        blended = 0.9 * propagated + teleport_part
        total_mass = lax.optimization_barrier(jnp.sum(blended * blended, axis=0))
        current = (blended / jnp.sqrt(0.05 + total_mass / VERTICES)).astype(jnp.bfloat16)
    return current
```

```python
import functools

import jax
import jax.numpy as jnp
from jax import lax
from jax.experimental import pallas as pl
from jax.experimental.pallas import tpu as pltpu
from jax.sharding import Mesh
from jax.sharding import PartitionSpec as P

ALL = ("y", "z", "c", "x")
LIMIT = 4 * 1024 * 1024
TILE = 128
ROWS_PER_STEP = 4

VMEM = pl.BlockSpec(memory_space=pltpu.VMEM)
SMEM = pl.BlockSpec(memory_space=pltpu.SMEM)
HBM = pl.BlockSpec(memory_space=pltpu.HBM)
PARAMS = pltpu.CompilerParams(vmem_limit_bytes=LIMIT)


def parities():
    return lax.axis_index("x") % 2, lax.axis_index("c")


def send_lists():
    p, q = parities()
    return ((p, 1 - p), (1 - p, p), (2 + q, 3 - q), (3 - q, 2 + q))


def pairings(count):
    near = [(i, i ^ 1) for i in range(count)]
    near_odd = [(i, (i + 1) % count if i % 2 else (i - 1) % count) for i in range(count)]
    far = [(i, i ^ 4) for i in range(count)]
    far_odd = [(i, (i + 4) % count if (i // 4) % 2 else (i - 4) % count) for i in range(count)]
    return near, near_odd, far, far_odd


def pack(halo, table, sends):
    for (to, _), send in zip(send_lists(), sends):
        for j in range(send.shape[0]):
            send[j] = table[halo[0, to, j]]


def first_kernel(halo, features, *sends_and_sems):
    *sends, sems = sends_and_sems
    copies = []
    for k, (to, _) in enumerate(send_lists()):
        for j in range(sends[k].shape[0]):
            copies.append(
                pltpu.make_async_copy(features.at[halo[0, to, j]], sends[k].at[j], sems.at[k, j])
            )
            copies[-1].start()
    for copy in copies:
        copy.wait()


def load_kernel(features, tiles, table, kept, sems):
    copies = [
        pltpu.make_async_copy(features, table.at[pl.ds(0, features.shape[0])], sems.at[0]),
        pltpu.make_async_copy(tiles, kept, sems.at[1]),
    ]
    for copy in copies:
        copy.start()
    for copy in copies:
        copy.wait()


def fold(rows):
    return jnp.sum(rows.reshape(rows.shape[0] // 8, 8, rows.shape[1]), axis=0)


def gather_halo(table, received, nblocks):
    for (_, source), block in zip(send_lists(), received):
        size = block.shape[0]
        table[pl.ds(nblocks + source * size, size)] = block[...]


def row_product(row, per_row, cols, tiles, table):
    acc = None
    for t in range(0, per_row, 2):
        at = row * per_row + t
        left = jnp.concatenate([tiles[at], tiles[at + 1]], axis=1)
        right = jnp.concatenate([table[cols[at]], table[cols[at + 1]]], axis=0)
        part = jnp.dot(left, right, preferred_element_type=jnp.float32)
        acc = part if acc is None else acc + part
    return acc


def over_rows(nblocks, count, body):
    def step(i, sums):
        for k in range(ROWS_PER_STEP):
            sums = body(i * ROWS_PER_STEP + k, sums)
        return sums

    zero = tuple(jnp.zeros((8, 256), jnp.float32) for _ in range(count))
    return lax.fori_loop(0, nblocks // ROWS_PER_STEP, step, zero)


def write_sums(out, sums):
    for k, s in enumerate(sums):
        out[pl.ds(k, 1), :] = jnp.sum(s, axis=0, keepdims=True)


def step1_kernel(cols, halo, tiles, _, ra, rb, rc, rd, table, table_out, held, sums_out, *sends):
    nblocks = held.shape[0]
    per_row = tiles.shape[0] // nblocks
    gather_halo(table, (ra, rb, rc, rd), nblocks)

    def body(row, sums):
        spread = row_product(row, per_row, cols, tiles, table)
        held[row] = spread
        start = table[row].astype(jnp.float32)
        table_out[row] = (0.9 * spread + 0.1 * start).astype(jnp.bfloat16)
        new = (start * start, spread * start, spread * spread)
        return tuple(s + fold(n) for s, n in zip(sums, new))

    write_sums(sums_out, over_rows(nblocks, 3, body))
    pack(halo, table_out, sends)


def step2_kernel(cols, halo, tiles, features, _, ra, rb, rc, rd, table, table_out, sums_out, *sends):
    nblocks = features.shape[0] // 2
    per_row = tiles.shape[0] // nblocks
    gather_halo(table, (ra, rb, rc, rd), nblocks)

    def body(row, sums):
        spread = row_product(row, per_row, cols, tiles, table)
        start = features[row].astype(jnp.float32)
        table_out[row] = spread.astype(jnp.bfloat16)
        new = (spread * spread, spread * start)
        return tuple(s + fold(n) for s, n in zip(sums, new))

    write_sums(sums_out, over_rows(nblocks, 2, body))
    pack(halo, table_out, sends)


def step3_kernel(cols, tiles, features, held, _, ra, rb, rc, rd, table, spread_out, sums_out):
    nblocks = held.shape[0]
    per_row = tiles.shape[0] // nblocks
    gather_halo(table, (ra, rb, rc, rd), nblocks)

    def body(row, sums):
        spread = row_product(row, per_row, cols, tiles, table)
        spread_out[row] = spread
        start = features[row].astype(jnp.float32)
        new = (spread * spread, spread * start, spread * held[row])
        return tuple(s + fold(n) for s, n in zip(sums, new))

    write_sums(sums_out, over_rows(nblocks, 3, body))


def last_kernel(vertices, sums, features, held, spread, out):
    total = jnp.sum(sums[...], axis=0)
    ff, yf, yy, ww, wf, vv, vf, vy = [total[k : k + 1] for k in range(8)]

    def scale(mass):
        return 1.0 / jnp.sqrt(0.05 + mass * (1.0 / vertices))

    s1 = scale(0.81 * yy + 0.18 * yf + 0.01 * ff)
    s2 = scale(0.81 * s1 * s1 * ww + 0.18 * s1 * wf + 0.01 * ff)
    inner = 0.81 * s1 * s1 * vv + 0.18 * s1 * vy + 0.01 * yy
    cross = 0.9 * s1 * vf + 0.1 * yf
    s3 = scale(0.81 * s2 * s2 * inner + 0.18 * s2 * cross + 0.01 * ff)
    a = 0.81 * s1 * s2 * s3
    b = 0.09 * s2 * s3
    c = 0.1 * s3

    def body(row, carry):
        start = features[row].astype(jnp.float32)
        out[row] = (a * spread[row] + b * held[row] + c * start).astype(jnp.bfloat16)
        return carry

    lax.fori_loop(0, out.shape[0], body, 0)


def in_hbm(array):
    return pltpu.with_memory_space_constraint(array, pltpu.HBM)


def exchange(sends):
    perms = pairings(lax.axis_size(ALL))
    return [lax.ppermute(s, ALL, p) for s, p in zip(sends, perms)]


def join_kernel(first, second, third, out):
    joined = jnp.concatenate([first[...], second[...], third[...]], axis=0)
    out[...] = jnp.broadcast_to(joined[None], out.shape)


def add_kernel(sums, out):
    out[...] = jnp.broadcast_to(jnp.sum(sums[...], axis=0)[None], out.shape)


def spread_sums(kernel, axes, *sums):
    count = lax.axis_size(axes)
    copies = pl.pallas_call(
        kernel,
        out_shape=pltpu.VMEM((count, 8, sums[0].shape[-1]), jnp.float32),
        in_specs=[VMEM] * len(sums),
        out_specs=VMEM,
        compiler_params=PARAMS,
        name="copies",
    )(*sums)
    return lax.all_to_all(copies, axes, 0, 0, tiled=True)


def local(features, tile_values, tile_cols, halo_rows):
    tile = tile_values.shape[1]
    classes = features.shape[1]
    nblocks = features.shape[0] // tile
    peers, slots = halo_rows.shape[1:]
    vertices = features.shape[0] * lax.axis_size(ALL)
    blocks = in_hbm(features.reshape(nblocks, tile, classes))
    halo_rows = in_hbm(halo_rows)
    tile_cols = in_hbm(tile_cols)
    table_shape = pltpu.VMEM((nblocks + peers * slots, tile, classes), jnp.bfloat16)
    send_shape = [pltpu.VMEM((slots, tile, classes), jnp.bfloat16)] * peers
    wide = pltpu.VMEM((nblocks, tile, classes), jnp.float32)

    def sums_shape(count):
        return pltpu.VMEM((count, classes), jnp.float32)

    sends = pl.pallas_call(
        first_kernel,
        out_shape=send_shape,
        in_specs=[SMEM, HBM],
        out_specs=[VMEM] * 4,
        scratch_shapes=[pltpu.SemaphoreType.DMA((peers, slots))],
        compiler_params=PARAMS,
        name="first",
    )(halo_rows, blocks)
    received = exchange(sends)
    table0, kept = pl.pallas_call(
        load_kernel,
        out_shape=[table_shape, pltpu.VMEM(tile_values.shape, tile_values.dtype)],
        in_specs=[HBM, HBM],
        out_specs=[VMEM, VMEM],
        scratch_shapes=[pltpu.SemaphoreType.DMA((2,))],
        compiler_params=PARAMS,
        name="load",
    )(blocks, in_hbm(tile_values))
    table0, table1, held, sums1, *sends = pl.pallas_call(
        step1_kernel,
        out_shape=[table_shape, table_shape, wide, sums_shape(3)] + send_shape,
        input_output_aliases={3: 0},
        in_specs=[SMEM, SMEM] + [VMEM] * 6,
        out_specs=[VMEM] * 8,
        compiler_params=PARAMS,
        name="step1",
    )(tile_cols, halo_rows, kept, table0, *received)
    received = exchange(sends)
    _, table2, sums2, *sends = pl.pallas_call(
        step2_kernel,
        out_shape=[table_shape, table_shape, sums_shape(2)] + send_shape,
        input_output_aliases={4: 0},
        in_specs=[SMEM, SMEM] + [VMEM] * 7,
        out_specs=[VMEM] * 7,
        compiler_params=PARAMS,
        name="step2",
    )(tile_cols, halo_rows, kept, table0, table1, *received)
    received = exchange(sends)
    _, spread, sums3 = pl.pallas_call(
        step3_kernel,
        out_shape=[table_shape, wide, sums_shape(3)],
        input_output_aliases={4: 0},
        in_specs=[SMEM] + [VMEM] * 8,
        out_specs=[VMEM] * 3,
        compiler_params=PARAMS,
        name="step3",
    )(tile_cols, kept, table0, held, table2, *received)
    sums = spread_sums(join_kernel, ("c", "x"), sums1, sums2, sums3)
    sums = spread_sums(add_kernel, ("y", "z"), sums)
    out = pl.pallas_call(
        functools.partial(last_kernel, vertices),
        out_shape=jax.ShapeDtypeStruct((nblocks, tile, classes), jnp.bfloat16),
        in_specs=[VMEM] * 4,
        out_specs=VMEM,
        compiler_params=PARAMS,
        name="last",
    )(sums, table0, held, spread)
    return out.reshape(features.shape)


def solution(mesh):
    groups, reps = mesh.devices.shape
    grid = Mesh(mesh.devices.reshape(4, groups // 8, 2, reps), ALL)
    return jax.shard_map(
        local,
        mesh=grid,
        in_specs=(P(ALL, None), P(ALL, None, None), P(ALL), P(ALL, None, None)),
        out_specs=P(ALL, None),
        check_vma=False,
    )
```

```python
import functools

import jax
import jax.numpy as jnp
from jax import lax
from jax.experimental import pallas as pl
from jax.experimental.pallas import tpu as pltpu
from jax.sharding import Mesh
from jax.sharding import PartitionSpec as P

ALL = ("y", "z", "c", "x")
LIMIT = 4 * 1024 * 1024
TILE = 128
ROWS_PER_STEP = 8

VMEM = pl.BlockSpec(memory_space=pltpu.VMEM)
SMEM = pl.BlockSpec(memory_space=pltpu.SMEM)
HBM = pl.BlockSpec(memory_space=pltpu.HBM)
PARAMS = pltpu.CompilerParams(vmem_limit_bytes=LIMIT)


def parities():
    return lax.axis_index("x") % 2, lax.axis_index("c")


def send_lists():
    p, q = parities()
    return ((p, 1 - p), (1 - p, p), (2 + q, 3 - q), (3 - q, 2 + q))


def pairings(count):
    near = [(i, i ^ 1) for i in range(count)]
    near_odd = [(i, (i + 1) % count if i % 2 else (i - 1) % count) for i in range(count)]
    far = [(i, i ^ 4) for i in range(count)]
    far_odd = [(i, (i + 4) % count if (i // 4) % 2 else (i - 4) % count) for i in range(count)]
    return near, near_odd, far, far_odd


def pack(halo, table, sends):
    for (to, _), send in zip(send_lists(), sends):
        for j in range(send.shape[0]):
            send[j] = table[halo[0, to, j]]


def first_kernel(halo, features, table, *sends_and_scratch):
    *sends, lists, sems = sends_and_scratch
    copies = [
        pltpu.make_async_copy(halo, lists, sems.at[0]),
        pltpu.make_async_copy(features, table.at[pl.ds(0, features.shape[0])], sems.at[1]),
    ]
    for copy in copies:
        copy.start()
    for copy in copies:
        copy.wait()
    pack(lists, table, sends)


def load_kernel(tiles, cols, halo, kept, cols_out, halo_out, sems):
    copies = [
        pltpu.make_async_copy(cols, cols_out, sems.at[0]),
        pltpu.make_async_copy(halo, halo_out, sems.at[1]),
        pltpu.make_async_copy(tiles, kept, sems.at[2]),
    ]
    for copy in copies:
        copy.start()
    for copy in copies:
        copy.wait()


def fold(rows):
    return jnp.sum(rows.reshape(rows.shape[0] // 8, 8, rows.shape[1]), axis=0)


def gather_halo(table, received, nblocks):
    for (_, source), block in zip(send_lists(), received):
        size = block.shape[0]
        table[pl.ds(nblocks + source * size, size)] = block[...]


def row_product(row, per_row, cols, tiles, table):
    acc = None
    for t in range(0, per_row, 2):
        at = row * per_row + t
        left = jnp.concatenate([tiles[at], tiles[at + 1]], axis=1)
        right = jnp.concatenate([table[cols[at]], table[cols[at + 1]]], axis=0)
        part = jnp.dot(left, right, preferred_element_type=jnp.float32)
        acc = part if acc is None else acc + part
    return acc


def over_rows(nblocks, count, body):
    def step(i, sums):
        for k in range(ROWS_PER_STEP):
            sums = body(i * ROWS_PER_STEP + k, sums)
        return sums

    zero = tuple(jnp.zeros((8, 256), jnp.float32) for _ in range(count))
    return lax.fori_loop(0, nblocks // ROWS_PER_STEP, step, zero)


def write_sums(out, sums, at=0):
    for k, s in enumerate(sums):
        out[pl.ds(at + k, 1), :] = jnp.sum(s, axis=0, keepdims=True)


def step1_kernel(cols, halo, tiles, _, ra, rb, rc, rd, table, table_out, held, sums_out, *sends):
    nblocks = held.shape[0]
    per_row = tiles.shape[0] // nblocks
    gather_halo(table, (ra, rb, rc, rd), nblocks)

    def body(row, sums):
        spread = row_product(row, per_row, cols, tiles, table)
        held[row] = spread
        start = table[row].astype(jnp.float32)
        table_out[row] = (0.9 * spread + 0.1 * start).astype(jnp.bfloat16)
        new = (start * start, spread * start, spread * spread)
        return tuple(s + fold(n) for s, n in zip(sums, new))

    write_sums(sums_out, over_rows(nblocks, 3, body))
    pack(halo, table_out, sends)


def step2_kernel(cols, halo, tiles, features, _, ra, rb, rc, rd, table, table_out, sums_out, *sends):
    nblocks = features.shape[0] // 2
    per_row = tiles.shape[0] // nblocks
    gather_halo(table, (ra, rb, rc, rd), nblocks)

    def body(row, sums):
        spread = row_product(row, per_row, cols, tiles, table)
        start = features[row].astype(jnp.float32)
        table_out[row] = spread.astype(jnp.bfloat16)
        new = (spread * spread, spread * start)
        return tuple(s + fold(n) for s, n in zip(sums, new))

    write_sums(sums_out, over_rows(nblocks, 2, body))
    pack(halo, table_out, sends)


def step3_kernel(cols, tiles, features, held, _, ra, rb, rc, rd, sums1, sums2, table, spread_out, sums_out):
    nblocks = held.shape[0]
    per_row = tiles.shape[0] // nblocks
    gather_halo(table, (ra, rb, rc, rd), nblocks)

    def body(row, sums):
        spread = row_product(row, per_row, cols, tiles, table)
        spread_out[row] = spread
        start = features[row].astype(jnp.float32)
        new = (spread * spread, spread * start, spread * held[row])
        return tuple(s + fold(n) for s, n in zip(sums, new))

    first, second = sums1.shape[0], sums2.shape[0]
    sums_out[pl.ds(0, first)] = sums1[...]
    sums_out[pl.ds(first, second)] = sums2[...]
    write_sums(sums_out, over_rows(nblocks, 3, body), first + second)


def last_kernel(vertices, sums, features, held, spread, out, staged, sems):
    total = jnp.sum(sums[...], axis=0)
    ff, yf, yy, ww, wf, vv, vf, vy = [total[k : k + 1] for k in range(8)]

    def scale(mass):
        return 1.0 / jnp.sqrt(0.05 + mass * (1.0 / vertices))

    s1 = scale(0.81 * yy + 0.18 * yf + 0.01 * ff)
    s2 = scale(0.81 * s1 * s1 * ww + 0.18 * s1 * wf + 0.01 * ff)
    inner = 0.81 * s1 * s1 * vv + 0.18 * s1 * vy + 0.01 * yy
    cross = 0.9 * s1 * vf + 0.1 * yf
    s3 = scale(0.81 * s2 * s2 * inner + 0.18 * s2 * cross + 0.01 * ff)
    a = 0.81 * s1 * s2 * s3
    b = 0.09 * s2 * s3
    c = 0.1 * s3

    copies = []
    size = out.shape[0] // sems.shape[0]
    for k in range(sems.shape[0]):
        for row in range(k * size, (k + 1) * size):
            start = features[row].astype(jnp.float32)
            staged[row] = (a * spread[row] + b * held[row] + c * start).astype(jnp.bfloat16)
        part = pl.ds(k * size, size)
        copies.append(pltpu.make_async_copy(staged.at[part], out.at[part], sems.at[k]))
        copies[-1].start()
    for copy in copies:
        copy.wait()


def in_hbm(array):
    return pltpu.with_memory_space_constraint(array, pltpu.HBM)


def exchange(sends):
    perms = pairings(lax.axis_size(ALL))
    return [lax.ppermute(s, ALL, p) for s, p in zip(sends, perms)]


def pair_kernel(own, partner, out):
    out[...] = jnp.broadcast_to((own[...] + partner[...])[None], out.shape)


def add_kernel(sums, out):
    out[...] = jnp.broadcast_to(jnp.sum(sums[...], axis=0)[None], out.shape)


def spread_sums(kernel, axes, *sums):
    count = lax.axis_size(axes)
    copies = pl.pallas_call(
        kernel,
        out_shape=pltpu.VMEM((count, 8, sums[0].shape[-1]), jnp.float32),
        in_specs=[VMEM] * len(sums),
        out_specs=VMEM,
        compiler_params=PARAMS,
        name="copies",
    )(*sums)
    return lax.all_to_all(copies, axes, 0, 0, tiled=True)


def local(features, tile_values, tile_cols, halo_rows):
    tile = tile_values.shape[1]
    classes = features.shape[1]
    nblocks = features.shape[0] // tile
    peers, slots = halo_rows.shape[1:]
    vertices = features.shape[0] * lax.axis_size(ALL)
    blocks = in_hbm(features.reshape(nblocks, tile, classes))
    halo_rows = in_hbm(halo_rows)
    tile_cols = in_hbm(tile_cols)
    table_shape = pltpu.VMEM((nblocks + peers * slots, tile, classes), jnp.bfloat16)
    send_shape = [pltpu.VMEM((slots, tile, classes), jnp.bfloat16)] * peers
    wide = pltpu.VMEM((nblocks, tile, classes), jnp.float32)

    def sums_shape(count):
        return pltpu.VMEM((count, classes), jnp.float32)

    table0, *sends = pl.pallas_call(
        first_kernel,
        out_shape=[table_shape] + send_shape,
        in_specs=[HBM, HBM],
        out_specs=[VMEM] * 5,
        scratch_shapes=[
            pltpu.SMEM(halo_rows.shape, jnp.int32),
            pltpu.SemaphoreType.DMA((2,)),
        ],
        compiler_params=PARAMS,
        name="first",
    )(halo_rows, blocks)
    received = exchange(sends)
    kept, tile_cols, halo_rows = pl.pallas_call(
        load_kernel,
        out_shape=[
            pltpu.VMEM(tile_values.shape, tile_values.dtype),
            pltpu.SMEM(tile_cols.shape, jnp.int32),
            pltpu.SMEM(halo_rows.shape, jnp.int32),
        ],
        in_specs=[HBM] * 3,
        out_specs=[VMEM, SMEM, SMEM],
        scratch_shapes=[pltpu.SemaphoreType.DMA((3,))],
        compiler_params=PARAMS,
        name="load",
    )(in_hbm(tile_values), tile_cols, halo_rows)
    table0, table1, held, sums1, *sends = pl.pallas_call(
        step1_kernel,
        out_shape=[table_shape, table_shape, wide, sums_shape(3)] + send_shape,
        input_output_aliases={3: 0},
        in_specs=[SMEM, SMEM] + [VMEM] * 6,
        out_specs=[VMEM] * 8,
        compiler_params=PARAMS,
        name="step1",
    )(tile_cols, halo_rows, kept, table0, *received)
    received = exchange(sends)
    _, table2, sums2, *sends = pl.pallas_call(
        step2_kernel,
        out_shape=[table_shape, table_shape, sums_shape(2)] + send_shape,
        input_output_aliases={4: 0},
        in_specs=[SMEM, SMEM] + [VMEM] * 7,
        out_specs=[VMEM] * 7,
        compiler_params=PARAMS,
        name="step2",
    )(tile_cols, halo_rows, kept, table0, table1, *received)
    received = exchange(sends)
    _, spread, sums = pl.pallas_call(
        step3_kernel,
        out_shape=[table_shape, wide, sums_shape(8)],
        input_output_aliases={4: 0},
        in_specs=[SMEM] + [VMEM] * 10,
        out_specs=[VMEM] * 3,
        compiler_params=PARAMS,
        name="step3",
    )(tile_cols, kept, table0, held, table2, *received, sums1, sums2)
    partner = lax.ppermute(sums, "c", [(0, 1), (1, 0)])
    sums = spread_sums(pair_kernel, ("y", "x"), sums, partner)
    sums = spread_sums(add_kernel, ("z",), sums)
    out = pl.pallas_call(
        functools.partial(last_kernel, vertices),
        out_shape=jax.ShapeDtypeStruct((nblocks, tile, classes), jnp.bfloat16),
        in_specs=[VMEM] * 4,
        out_specs=HBM,
        scratch_shapes=[
            pltpu.VMEM((nblocks, tile, classes), jnp.bfloat16),
            pltpu.SemaphoreType.DMA((4,)),
        ],
        compiler_params=PARAMS,
        name="last",
    )(sums, table0, held, spread)
    return out.reshape(features.shape)


def solution(mesh):
    groups, reps = mesh.devices.shape
    grid = Mesh(mesh.devices.reshape(4, groups // 8, 2, reps), ALL)
    return jax.shard_map(
        local,
        mesh=grid,
        in_specs=(P(ALL, None), P(ALL, None, None), P(ALL), P(ALL, None, None)),
        out_specs=P(ALL, None),
        check_vma=False,
    )
```

```python
import functools

import jax
import jax.numpy as jnp
from jax import lax
from jax.experimental import pallas as pl
from jax.experimental.pallas import tpu as pltpu
from jax.sharding import Mesh
from jax.sharding import PartitionSpec as P

ALL = ("y", "z", "c", "x")
LIMIT = 4 * 1024 * 1024
TILE = 128
EARLY_ROWS = 8
LATE_ROWS = 16

VMEM = pl.BlockSpec(memory_space=pltpu.VMEM)
SMEM = pl.BlockSpec(memory_space=pltpu.SMEM)
HBM = pl.BlockSpec(memory_space=pltpu.HBM)
PARAMS = pltpu.CompilerParams(vmem_limit_bytes=LIMIT)


def parities():
    return lax.axis_index("x") % 2, lax.axis_index("c")


def send_lists():
    p, q = parities()
    return ((p, 1 - p), (1 - p, p), (2 + q, 3 - q), (3 - q, 2 + q))


def pairings(count):
    near = [(i, i ^ 1) for i in range(count)]
    near_odd = [(i, (i + 1) % count if i % 2 else (i - 1) % count) for i in range(count)]
    far = [(i, i ^ 4) for i in range(count)]
    far_odd = [(i, (i + 4) % count if (i // 4) % 2 else (i - 4) % count) for i in range(count)]
    return near, near_odd, far, far_odd


def pack(halo, table, sends):
    for (to, _), send in zip(send_lists(), sends):
        for j in range(send.shape[0]):
            send[j] = table[halo[0, to, j]]


def first_kernel(halo, features, table, *sends_and_scratch):
    *sends, lists, sems = sends_and_scratch
    nblocks = features.shape[0]
    copies = [
        pltpu.make_async_copy(halo, lists, sems.at[0]),
        pltpu.make_async_copy(features, table.at[pl.ds(0, nblocks)], sems.at[1]),
    ]
    for copy in copies:
        copy.start()
    clear_last(table)
    for copy in copies:
        copy.wait()
    pack(lists, table, sends)


def clear_last(table):
    last = table.shape[0] - 1
    table[last] = jnp.zeros(table.shape[1:], table.dtype)


def load_kernel(nblocks, tiles, cols, halo, kept, early, late, late_tile, most, halo_out, slots, sems):
    per_row = cols.shape[0] // nblocks
    per_peer = halo.shape[2]
    zero = nblocks + halo.shape[1] * per_peer
    copies = [
        pltpu.make_async_copy(cols, slots, sems.at[0]),
        pltpu.make_async_copy(halo, halo_out, sems.at[1]),
        pltpu.make_async_copy(tiles, kept, sems.at[2]),
    ]
    for copy in copies:
        copy.start()
    copies[0].wait()
    lists = send_lists()
    starts = [nblocks + lists[k][1] * per_peer for k in (1, 3)]

    def row_body(row, top):
        count = jnp.int32(0)
        for t in range(per_row):
            at = row * per_row + t
            slot = slots[at]
            is_late = False
            for start in starts:
                is_late |= (slot >= start) & (slot < start + per_peer)
            early[at] = jnp.where(is_late, zero, slot)
            late[at] = zero
            late_tile[at] = at
            late[row * per_row + count] = jnp.where(is_late, slot, zero)
            late_tile[row * per_row + count] = at
            count += is_late.astype(jnp.int32)
        return jnp.maximum(top, count)

    most[0] = lax.fori_loop(0, nblocks, row_body, jnp.int32(0))
    for copy in copies[1:]:
        copy.wait()


def fold(rows):
    return jnp.sum(rows.reshape(rows.shape[0] // 8, 8, rows.shape[1]), axis=0)


def gather_halo(table, received, which, nblocks):
    lists = send_lists()
    for k, block in zip(which, received):
        size = block.shape[0]
        table[pl.ds(nblocks + lists[k][1] * size, size)] = block[...]


def product(places, tiles, table):
    acc = None
    for (t0, s0), (t1, s1) in zip(places[::2], places[1::2]):
        left = jnp.concatenate([tiles[t0], tiles[t1]], axis=1)
        right = jnp.concatenate([table[s0], table[s1]], axis=0)
        part = jnp.dot(left, right, preferred_element_type=jnp.float32)
        acc = part if acc is None else acc + part
    return acc


def over_rows(nblocks, unroll, count, body):
    def step(i, sums):
        for k in range(unroll):
            sums = body(i * unroll + k, sums)
        return sums

    zero = tuple(jnp.zeros((8, 256), jnp.float32) for _ in range(count))
    if unroll == nblocks:
        return step(0, zero)
    return lax.fori_loop(0, nblocks // unroll, step, zero)


def write_sums(out, sums, at=0):
    for k, s in enumerate(sums):
        out[pl.ds(at + k, 1), :] = jnp.sum(s, axis=0, keepdims=True)


def early_rows(early, tiles, table, acc, count, grams):
    nblocks = acc.shape[0]
    per_row = tiles.shape[0] // nblocks

    def body(row, sums):
        first = row * per_row
        acc[row] = product([(first + t, early[first + t]) for t in range(per_row)], tiles, table)
        return tuple(s + fold(n) for s, n in zip(sums, grams(row)))

    return over_rows(nblocks, EARLY_ROWS, count, body)


def late_rows(late, late_tile, most, tiles, table, acc, count, finish):
    nblocks = acc.shape[0]
    per_row = tiles.shape[0] // nblocks
    half = per_row // 2

    def part(row, begin):
        at = row * per_row + begin
        return product([(late_tile[at + t], late[at + t]) for t in range(half)], tiles, table)

    @pl.when(most[0] > half)
    def _():
        def rest(row, carry):
            acc[row] += part(row, half)
            return carry

        lax.fori_loop(0, nblocks, rest, 0)

    def body(row, sums):
        spread = acc[row] + part(row, 0)
        acc[row] = spread
        return tuple(s + fold(n) for s, n in zip(sums, finish(row, spread)))

    return over_rows(nblocks, LATE_ROWS, count, body)


def early1_kernel(early, tiles, _, ra, rc, table, acc):
    gather_halo(table, (ra, rc), (0, 2), acc.shape[0])
    early_rows(early, tiles, table, acc, 0, lambda row: ())


def early2_kernel(early, tiles, features, held, _, ra, rc, table, acc, sums_out):
    gather_halo(table, (ra, rc), (0, 2), acc.shape[0])

    def grams(row):
        start, spread = features[row].astype(jnp.float32), held[row]
        return start * start, spread * start, spread * spread

    write_sums(sums_out, early_rows(early, tiles, table, acc, 3, grams))


def early3_kernel(early, tiles, features, held, _, ra, rc, table, acc, sums_out):
    gather_halo(table, (ra, rc), (0, 2), acc.shape[0])

    def grams(row):
        start, spread = features[row].astype(jnp.float32), held[row]
        return spread * spread, spread * start

    write_sums(sums_out, early_rows(early, tiles, table, acc, 2, grams))


def late1_kernel(late, late_tile, most, halo, tiles, _, __, rb, rd, table, acc, table_out, *sends):
    gather_halo(table, (rb, rd), (1, 3), acc.shape[0])
    clear_last(table_out)

    def finish(row, spread):
        start = table[row].astype(jnp.float32)
        table_out[row] = (0.9 * spread + 0.1 * start).astype(jnp.bfloat16)
        return ()

    late_rows(late, late_tile, most, tiles, table, acc, 0, finish)
    pack(halo, table_out, sends)


def late2_kernel(late, late_tile, most, halo, tiles, _, __, rb, rd, table, acc, table_out, *sends):
    gather_halo(table, (rb, rd), (1, 3), acc.shape[0])
    clear_last(table_out)

    def finish(row, spread):
        table_out[row] = spread.astype(jnp.bfloat16)
        return ()

    late_rows(late, late_tile, most, tiles, table, acc, 0, finish)
    pack(halo, table_out, sends)


def late3_kernel(late, late_tile, most, tiles, features, held, sums1, sums2, _, __, rb, rd, table, acc, sums_out):
    gather_halo(table, (rb, rd), (1, 3), acc.shape[0])
    first, second = sums1.shape[0], sums2.shape[0]
    sums_out[pl.ds(0, first)] = sums1[...]
    sums_out[pl.ds(first, second)] = sums2[...]

    def finish(row, spread):
        start = features[row].astype(jnp.float32)
        return spread * spread, spread * start, spread * held[row]

    sums = late_rows(late, late_tile, most, tiles, table, acc, 3, finish)
    write_sums(sums_out, sums, first + second)


def last_kernel(vertices, sums, features, held, spread, out, staged, sems):
    total = jnp.sum(sums[...], axis=0)
    ff, yf, yy, ww, wf, vv, vf, vy = [total[k : k + 1] for k in range(8)]

    def scale(mass):
        return 1.0 / jnp.sqrt(0.05 + mass * (1.0 / vertices))

    s1 = scale(0.81 * yy + 0.18 * yf + 0.01 * ff)
    s2 = scale(0.81 * s1 * s1 * ww + 0.18 * s1 * wf + 0.01 * ff)
    inner = 0.81 * s1 * s1 * vv + 0.18 * s1 * vy + 0.01 * yy
    cross = 0.9 * s1 * vf + 0.1 * yf
    s3 = scale(0.81 * s2 * s2 * inner + 0.18 * s2 * cross + 0.01 * ff)
    a = 0.81 * s1 * s2 * s3
    b = 0.09 * s2 * s3
    c = 0.1 * s3

    copies = []
    size = out.shape[0] // sems.shape[0]
    for k in range(sems.shape[0]):
        for row in range(k * size, (k + 1) * size):
            start = features[row].astype(jnp.float32)
            staged[row] = (a * spread[row] + b * held[row] + c * start).astype(jnp.bfloat16)
        part = pl.ds(k * size, size)
        copies.append(pltpu.make_async_copy(staged.at[part], out.at[part], sems.at[k]))
        copies[-1].start()
    for copy in copies:
        copy.wait()


def in_hbm(array):
    return pltpu.with_memory_space_constraint(array, pltpu.HBM)


def call(kernel, name, shapes, aliases, scalars, arrays):
    return pl.pallas_call(
        kernel,
        out_shape=shapes,
        in_specs=[SMEM] * len(scalars) + [VMEM] * len(arrays),
        out_specs=[VMEM] * len(shapes),
        input_output_aliases=aliases,
        compiler_params=PARAMS,
        name=name,
    )(*scalars, *arrays)


def exchange(sends):
    perms = pairings(lax.axis_size(ALL))
    return [lax.ppermute(s, ALL, p) for s, p in zip(sends, perms)]


def pair_kernel(own, partner, out):
    out[...] = jnp.broadcast_to((own[...] + partner[...])[None], out.shape)


def add_kernel(sums, out):
    out[...] = jnp.broadcast_to(jnp.sum(sums[...], axis=0)[None], out.shape)


def spread_sums(kernel, axes, *sums):
    count = lax.axis_size(axes)
    copies = pl.pallas_call(
        kernel,
        out_shape=pltpu.VMEM((count, 8, sums[0].shape[-1]), jnp.float32),
        in_specs=[VMEM] * len(sums),
        out_specs=VMEM,
        compiler_params=PARAMS,
        name="copies",
    )(*sums)
    return lax.all_to_all(copies, axes, 0, 0, tiled=True)


def local(features, tile_values, tile_cols, halo_rows):
    tile = tile_values.shape[1]
    classes = features.shape[1]
    nblocks = features.shape[0] // tile
    peers, slots = halo_rows.shape[1:]
    vertices = features.shape[0] * lax.axis_size(ALL)
    blocks = in_hbm(features.reshape(nblocks, tile, classes))
    halo_rows = in_hbm(halo_rows)
    tile_cols = in_hbm(tile_cols)
    table_shape = pltpu.VMEM((nblocks + peers * slots + 1, tile, classes), jnp.bfloat16)
    send_shape = [pltpu.VMEM((slots, tile, classes), jnp.bfloat16)] * peers
    wide = pltpu.VMEM((nblocks, tile, classes), jnp.float32)

    def sums_shape(count):
        return pltpu.VMEM((count, classes), jnp.float32)

    table0, *sends = pl.pallas_call(
        first_kernel,
        out_shape=[table_shape] + send_shape,
        in_specs=[HBM, HBM],
        out_specs=[VMEM] * 5,
        scratch_shapes=[
            pltpu.SMEM(halo_rows.shape, jnp.int32),
            pltpu.SemaphoreType.DMA((2,)),
        ],
        compiler_params=PARAMS,
        name="first",
    )(halo_rows, blocks)
    ra, rb, rc, rd = exchange(sends)
    table_list = pltpu.SMEM(tile_cols.shape, jnp.int32)
    kept, early, late, late_tile, most, halo_rows = pl.pallas_call(
        functools.partial(load_kernel, nblocks),
        out_shape=[
            pltpu.VMEM(tile_values.shape, tile_values.dtype),
            table_list,
            table_list,
            table_list,
            pltpu.SMEM((1,), jnp.int32),
            pltpu.SMEM(halo_rows.shape, jnp.int32),
        ],
        in_specs=[HBM] * 3,
        out_specs=[VMEM] + [SMEM] * 5,
        scratch_shapes=[pltpu.SMEM(tile_cols.shape, jnp.int32), pltpu.SemaphoreType.DMA((3,))],
        compiler_params=PARAMS,
        name="load",
    )(in_hbm(tile_values), tile_cols, halo_rows)
    lists = (late, late_tile, most)
    table0, held = call(
        early1_kernel, "early1", [table_shape, wide], {2: 0}, [early], [kept, table0, ra, rc]
    )
    table0, held, table1, *sends = call(
        late1_kernel,
        "late1",
        [table_shape, wide, table_shape] + send_shape,
        {5: 0, 6: 1},
        [*lists, halo_rows],
        [kept, table0, held, rb, rd],
    )
    ra, rb, rc, rd = exchange(sends)
    table1, spread, sums1 = call(
        early2_kernel,
        "early2",
        [table_shape, wide, sums_shape(3)],
        {4: 0},
        [early],
        [kept, table0, held, table1, ra, rc],
    )
    _, spread2, table2, *sends = call(
        late2_kernel,
        "late2",
        [table_shape, wide, table_shape] + send_shape,
        {5: 0, 6: 1},
        [*lists, halo_rows],
        [kept, table1, spread, rb, rd],
    )
    ra, rb, rc, rd = exchange(sends)
    table2, spread, sums2 = call(
        early3_kernel,
        "early3",
        [table_shape, wide, sums_shape(2)],
        {4: 0},
        [early],
        [kept, table0, spread2, table2, ra, rc],
    )
    _, spread, sums = call(
        late3_kernel,
        "late3",
        [table_shape, wide, sums_shape(8)],
        {8: 0, 9: 1},
        lists,
        [kept, table0, held, sums1, sums2, table2, spread, rb, rd],
    )
    partner = lax.ppermute(sums, "c", [(0, 1), (1, 0)])
    sums = spread_sums(pair_kernel, ("y", "x"), sums, partner)
    sums = spread_sums(add_kernel, ("z",), sums)
    out = pl.pallas_call(
        functools.partial(last_kernel, vertices),
        out_shape=jax.ShapeDtypeStruct((nblocks, tile, classes), jnp.bfloat16),
        in_specs=[VMEM] * 4,
        out_specs=HBM,
        scratch_shapes=[
            pltpu.VMEM((nblocks, tile, classes), jnp.bfloat16),
            pltpu.SemaphoreType.DMA((4,)),
        ],
        compiler_params=PARAMS,
        name="last",
    )(sums, table0, held, spread)
    return out.reshape(features.shape)


def solution(mesh):
    groups, reps = mesh.devices.shape
    grid = Mesh(mesh.devices.reshape(4, groups // 8, 2, reps), ALL)
    return jax.shard_map(
        local,
        mesh=grid,
        in_specs=(P(ALL, None), P(ALL, None, None), P(ALL), P(ALL, None, None)),
        out_specs=P(ALL, None),
        check_vma=False,
    )
```
